256 devices in a mesh: seq: 16 (over y, x), row: 4 (over z_lo, core), col: 4 (over z_hi).
Axes of the slice: x: 4, y: 4, z: 8 (z_hi: 4, z_lo: 2; z = z_hi * 2 + z_lo), core: 2. Of those that a mesh axis runs over, the one named last changes fastest.
Arguments:
- activations: bfloat16 [16, 64, 8192], P(None, 'row', 'seq'), may hold values from -6 to 6
- gradients: bfloat16 [16, 64, 8192], P(None, 'col', 'seq'), may hold values from -6 to 6
- basis_in: bfloat16 [8192, 4096], P('seq', 'col'), may hold values from -0.0625 to 0.0625
- basis_out: bfloat16 [8192, 4096], P('seq', 'row'), may hold values from -0.0625 to 0.0625
- lengths: int32 [16], replicated, may hold values from 16 to 64
Outputs:
- corrections: float32 [4096, 4096], P(('row', 'seq'), 'col')
The draws below stay inside these ranges and needn't reach their ends.
All inputs are finite; a program needn't handle non-finite values.
Results may differ from the reference program's by a relative error of at most 0.0023.
Values may be sent and summed in bfloat16 or wider, within the bound.
A program may use at most 64 MiB of HBM per device.

```python
import jax
import jax.numpy as jnp
from jax import lax

FEAT_IN = 8192
FEAT_OUT = 8192
DIRS_IN = 4096
DIRS_OUT = 4096
MAXLEN = 64
SEQS = 16


def set_ends(array, own_key, low, high):
    dims = array.shape
    index_at = [jax.random.randint(jax.random.fold_in(own_key, axis), (), 0, dims[axis]) for axis in range(len(dims))]
    array = array.at[tuple(index_at)].set(low)
    longest = dims.index(max(dims))
    index_at[longest] = (index_at[longest] + 1) % dims[longest]
    return array.at[tuple(index_at)].set(high)


def block_levels(key, extent, shards, low, high):
    def one(position, parts):
        heights = jax.random.uniform(jax.random.fold_in(jax.random.fold_in(key, 6), position), (parts,), jnp.float32, low / len(shards), high / len(shards))
        return jnp.repeat(jnp.exp(heights), extent[position] // parts).reshape((-1,) + (1,) * (len(extent) - position - 1))

    loudness = one(*shards[0])
    for cut in shards[1:]:
        loudness = loudness * one(*cut)
    return loudness


def centred(stream_key, extent, width, bound, shards=(), held_as=jnp.bfloat16):
    drawn = width * jax.random.normal(stream_key, extent, jnp.float32)
    if shards:
        drawn = drawn * block_levels(stream_key, extent, shards, -0.22, 0.18)
    return jnp.clip(drawn, -bound, bound).astype(held_as)


def setup_inputs(seed: int = 0) -> dict:
    keys = jax.random.split(jax.random.key(seed), 6)
    activations = centred(keys[0], (SEQS, MAXLEN, FEAT_IN), 1.0, 6.0, ((1, 4), (2, 16)))
    gradients = centred(keys[1], (SEQS, MAXLEN, FEAT_OUT), 1.0, 6.0, ((1, 4), (2, 16)))
    basis_in = centred(keys[2], (FEAT_IN, DIRS_IN), FEAT_IN ** -0.5, 0.0625, ((0, 16), (1, 4)))
    basis_out = centred(keys[3], (FEAT_OUT, DIRS_OUT), FEAT_OUT ** -0.5, 0.0625, ((0, 16), (1, 4)))
    lengths = set_ends(jax.random.randint(keys[4], (SEQS,), MAXLEN // 4, MAXLEN + 1), jax.random.fold_in(keys[4], 1), MAXLEN // 4, MAXLEN).astype(jnp.int32)
    return {"activations": activations, "gradients": gradients, "basis_in": basis_in, "basis_out": basis_out, "lengths": lengths}


def reference(activations, gradients, basis_in, basis_out, lengths):
    slots = jnp.arange(MAXLEN).astype(jnp.int32)

    def one_sequence(total, index):
        turned_in = jnp.dot(activations[index], basis_in, preferred_element_type=jnp.float32).astype(jnp.bfloat16)
        turned_out = jnp.dot(gradients[index], basis_out, preferred_element_type=jnp.float32).astype(jnp.bfloat16)
        live_rows = slots < lengths[index]
        kept = jnp.where(live_rows[:, None], turned_out, jnp.zeros((), jnp.bfloat16))
        product_tile = lax.dot_general(kept, turned_in, (((0,), (0,)), ((), ())), preferred_element_type=jnp.float32)
        return total + product_tile * product_tile, None

    start_total = jnp.zeros((DIRS_OUT, DIRS_IN), jnp.float32)
    total, unused = lax.scan(one_sequence, start_total, jnp.arange(SEQS).astype(jnp.int32))
    return total / (SEQS * MAXLEN)
```

```python
import functools

import jax
import jax.numpy as jnp
from jax import lax
from jax.experimental import pallas as pl
from jax.experimental.pallas import tpu as pltpu
from jax.sharding import PartitionSpec as P

MESH = pl.DeviceIdType.MESH
F32 = jnp.float32
BF16 = jnp.bfloat16

PHASES = dict(rs1_in=6, rs1_out=6, rs2_in=3, rs2_out=3, row=3, ag1=4, ag2=4, z=3, fwd=4, last=1)
FIRST = {}
TOTAL = 0
for _name, _count in PHASES.items():
    FIRST[_name] = TOTAL
    TOTAL += _count


def kernel(
    act_hbm, grad_hbm, bin_hbm, bout_hbm, len_ref, out_ref,
    act, grad, bin_, bout,
    p32_in, p16_in, p32_out, p16_out,
    got_in, got_out, tmp_in, tmp_out,
    q_in, q_out, got2_in, got2_out,
    t_in, gbuf, obuf, lhs, acc, xch,
    load_sem, send_sem, recv_sem,
):
    s = lax.axis_index("seq")
    r = lax.axis_index("row")
    c = lax.axis_index("col")
    y, x = lax.div(s, 4), lax.rem(s, 4)
    zl, k = lax.div(r, 2), lax.rem(r, 2)
    a = x + k * (y - x)
    b = y + k * (x - y)
    step_a, step_b = 1 + 3 * k, 4 - 3 * k

    def turn(v):
        return lax.rem(v + 4, 4)

    def at(a_, b_):
        return a_ * step_a + b_ * step_b

    def send(name, i, src, dst, device):
        n = FIRST[name] + i
        copy = pltpu.make_async_remote_copy(
            src_ref=src, dst_ref=dst, send_sem=send_sem.at[n], recv_sem=recv_sem.at[n],
            device_id=device, device_id_type=MESH,
        )
        copy.start()
        return copy

    loads = [
        pltpu.make_async_copy(src, dst, load_sem.at[i])
        for i, (src, dst) in enumerate(
            [(act_hbm, act), (bin_hbm, bin_), (grad_hbm, grad), (bout_hbm, bout)]
        )
    ]
    for load in loads:
        load.start()

    barrier = pltpu.get_barrier_semaphore()
    peers = []
    for d in (1, 2, 3):
        peers.append((at(turn(a + d), b), r, c))
        peers.append((at(a, turn(b + d)), r, c))
        peers.append((s, lax.rem(r + d, 4), c))
        peers.append((s, r, lax.rem(c + d, 4)))
    for peer in peers:
        pl.semaphore_signal(barrier, inc=1, device_id=peer, device_id_type=MESH)

    ap, am, a2 = turn(a + 1), turn(a - 1), turn(a + 2)
    bp, bm, b2 = turn(b + 1), turn(b - 1), turn(b + 2)
    right, left = (at(ap, b), r, c), (at(am, b), r, c)

    loads[0].wait()
    loads[1].wait()
    for j in range(4):
        m = jnp.dot(act[...], bin_[:, 256 * j : 256 * (j + 1)], preferred_element_type=F32)
        for i in range(4):
            blk = m[64 * i : 64 * (i + 1)]
            at_blk = i * step_a + j * step_b
            p32_in[at_blk] = blk
            p16_in[at_blk] = blk.astype(BF16)

    pl.semaphore_wait(barrier, len(peers))

    def ring1_start(name, p16, got):
        return [
            send(name, 0, p16.at[pl.ds(a2 * 4, 2)], got.at[0], right),
            send(name, 1, p16.at[pl.ds(a2 * 4 + 2, 2)], got.at[1], left),
            send(name, 2, p16.at[pl.ds(ap * 4 + 2, 2)], got.at[2], right),
            send(name, 3, p16.at[pl.ds(am * 4, 2)], got.at[3], left),
        ]

    def ring1_relay(name, copies, p32, got, tmp):
        copies[0].wait_recv()
        tmp[0] = (got[0].astype(F32) + p32[pl.ds(ap * 4, 2)]).astype(BF16)
        copies.append(send(name, 4, tmp.at[0], got.at[4], right))
        copies[1].wait_recv()
        tmp[1] = (got[1].astype(F32) + p32[pl.ds(am * 4 + 2, 2)]).astype(BF16)
        copies.append(send(name, 5, tmp.at[1], got.at[5], left))

    def ring1_end(copies, p32, got, q):
        copies[2].wait_recv()
        copies[3].wait_recv()
        copies[4].wait_recv()
        copies[5].wait_recv()
        q[0:2] = p32[pl.ds(a * 4, 2)] + got[3].astype(F32) + got[4].astype(F32)
        q[2:4] = p32[pl.ds(a * 4 + 2, 2)] + got[2].astype(F32) + got[5].astype(F32)

    def ring2_start(name, q, got2):
        return [
            send(name, d - 1, q.at[turn(b + d)], got2.at[d - 1], (at(a, turn(b + d)), r, c))
            for d in (2, 1, 3)
        ]

    def ring2_end(copies, q, got2):
        for copy in copies:
            copy.wait_recv()
        return q[b] + got2[0] + got2[1] + got2[2]

    pending = []
    rs1_in = ring1_start("rs1_in", p16_in, got_in)

    loads[2].wait()
    loads[3].wait()
    for j in range(4):
        m = jnp.dot(grad[...], bout[:, 256 * j : 256 * (j + 1)], preferred_element_type=F32)
        m = m.T
        for i in range(4):
            blk = m[64 * i : 64 * (i + 1)]
            at_blk = i * step_b + j * step_a
            p32_out[at_blk] = blk
            p16_out[at_blk] = blk.astype(BF16)
    rs1_out = ring1_start("rs1_out", p16_out, got_out)

    ring1_relay("rs1_in", rs1_in, p32_in, got_in, tmp_in)
    ring1_relay("rs1_out", rs1_out, p32_out, got_out, tmp_out)

    ring1_end(rs1_in, p32_in, got_in, q_in)
    rs2_in = ring2_start("rs2_in", q_in, got2_in)
    ring1_end(rs1_out, p32_out, got_out, q_out)
    rs2_out = ring2_start("rs2_out", q_out, got2_out)

    turned = ring2_end(rs2_in, q_in, got2_in).astype(BF16)
    t_in[0] = turned[:, :128]
    t_in[1] = turned[:, 128:]
    gbuf[a, b, r] = t_in[k]
    row = [
        send("row", 0, t_in.at[1 - k], gbuf.at[b, a, r], (s, 2 * zl + 1 - k, c)),
        send("row", 1, t_in.at[k], gbuf.at[a, b, r], (s, 2 * (1 - zl) + k, c)),
        send("row", 2, t_in.at[1 - k], gbuf.at[b, a, r], (s, 2 * (1 - zl) + 1 - k, c)),
    ]

    obuf[k, c] = ring2_end(rs2_out, q_out, got2_out).astype(BF16)
    partner = (s, 2 * zl + 1 - k, c)
    z = [
        send("z", d - 1, obuf.at[k, c], obuf.at[k, c], (s, r, turn(c + d)))
        for d in (2, 1, 3)
    ]
    fwd = [send("fwd", 0, obuf.at[k, c], obuf.at[k, c], partner)]

    for copy in row:
        copy.wait_recv()
    right_b, left_b = (at(a, bp), r, c), (at(a, bm), r, c)
    ag1 = [
        send("ag1", 0, gbuf.at[a, b], gbuf.at[a, b], right_b),
        send("ag1", 1, gbuf.at[a, b], gbuf.at[a, b], left_b),
    ]
    ag1[0].wait_recv()
    ag1.append(send("ag1", 2, gbuf.at[a, bm, pl.ds(0, 2)], gbuf.at[a, bm, pl.ds(0, 2)], right_b))
    ag1[1].wait_recv()
    ag1.append(send("ag1", 3, gbuf.at[a, bp, pl.ds(2, 2)], gbuf.at[a, bp, pl.ds(2, 2)], left_b))
    ag1[2].wait_recv()
    ag1[3].wait_recv()
    ag2 = [
        send("ag2", 0, gbuf.at[a], gbuf.at[a], right),
        send("ag2", 1, gbuf.at[a], gbuf.at[a], left),
    ]

    for i, d in enumerate((2, 1, 3)):
        z[i].wait_recv()
        from_ = turn(c - d)
        fwd.append(send("fwd", i + 1, obuf.at[k, from_], obuf.at[k, from_], partner))
    for copy in fwd:
        copy.wait_recv()

    lane = lax.broadcasted_iota(jnp.int32, (64, 256), 1)
    seq4 = lax.rem(lax.div(lane, 16), 4)
    slot = lax.div(lane, 64) * 16 + lax.rem(lane, 16)
    for g in range(4):
        keep = [
            jnp.logical_and(seq4 == i, slot < len_ref[4 * g + i]) for i in range(4)
        ]
        for kk in range(2):
            whole = jnp.concatenate(
                [obuf[kk, zz].astype(F32)[:, 64 * g : 64 * (g + 1)] for zz in range(4)], axis=1
            )
            for i in range(4):
                lhs[g, kk, i] = jnp.where(keep[i], whole, 0.0).astype(BF16)

    acc[...] = jnp.zeros_like(acc)

    def use(a_):
        for b_ in range(4):
            gy = b_ + k * (a_ - b_)
            gx = a_ + k * (b_ - a_)
            prod = jnp.dot(
                lhs[gy].reshape(512, 256), gbuf[a_, b_].reshape(256, 128),
                preferred_element_type=F32,
            )
            acc[:, gx] += jnp.sum((prod * prod).reshape(2, 4, 64, 128), axis=1)

    use(a)
    ag2[0].wait_recv()
    ag2.append(send("ag2", 2, gbuf.at[am, pl.ds(0, 2)], gbuf.at[am, pl.ds(0, 2)], right))
    ag2[1].wait_recv()
    ag2.append(send("ag2", 3, gbuf.at[ap, pl.ds(2, 2)], gbuf.at[ap, pl.ds(2, 2)], left))
    use(am)
    use(ap)
    ag2[2].wait_recv()
    ag2[3].wait_recv()
    use(a2)

    acc[...] = acc[...] * (1.0 / 1024.0)
    last = [send("last", 0, acc.at[1 - k], xch, partner)]
    for g in range(4):
        out_ref[:, pl.ds(pl.multiple_of(g * 256 + k * 128, 128), 128)] = acc[k, g]
    last[0].wait_recv()
    for g in range(4):
        out_ref[:, pl.ds(pl.multiple_of(g * 256 + (1 - k) * 128, 128), 128)] = xch[g]

    for copies in (rs1_in, rs1_out, rs2_in, rs2_out, row, z, fwd, ag1, ag2, last):
        for copy in copies:
            copy.wait_send()


def local(activations, gradients, basis_in, basis_out, lengths):
    any_ = pl.BlockSpec(memory_space=pl.ANY)
    vm = pltpu.VMEM
    return pl.pallas_call(
        kernel,
        out_shape=jax.ShapeDtypeStruct((64, 1024), F32),
        in_specs=[any_] * 4 + [pl.BlockSpec(memory_space=pltpu.SMEM)],
        out_specs=pl.BlockSpec(memory_space=pltpu.VMEM),
        scratch_shapes=[
            vm((256, 512), BF16), vm((256, 512), BF16),
            vm((512, 1024), BF16), vm((512, 1024), BF16),
            vm((16, 64, 256), F32), vm((16, 64, 256), BF16),
            vm((16, 64, 256), F32), vm((16, 64, 256), BF16),
            vm((6, 2, 64, 256), BF16), vm((6, 2, 64, 256), BF16),
            vm((2, 2, 64, 256), BF16), vm((2, 2, 64, 256), BF16),
            vm((4, 64, 256), F32), vm((4, 64, 256), F32),
            vm((3, 64, 256), F32), vm((3, 64, 256), F32),
            vm((2, 64, 128), BF16),
            vm((4, 4, 4, 64, 128), BF16),
            vm((2, 4, 64, 256), BF16),
            vm((4, 2, 4, 64, 256), BF16),
            vm((2, 4, 64, 128), F32),
            vm((4, 64, 128), F32),
            pltpu.SemaphoreType.DMA((4,)),
            pltpu.SemaphoreType.DMA((TOTAL,)),
            pltpu.SemaphoreType.DMA((TOTAL,)),
        ],
        compiler_params=pltpu.CompilerParams(
            collective_id=0, has_side_effects=True, vmem_limit_bytes=40 * 1024 * 1024
        ),
    )(
        activations.reshape(256, 512), gradients.reshape(256, 512),
        basis_in, basis_out, lengths,
    )


def solution(mesh):
    return jax.shard_map(
        local,
        mesh=mesh,
        in_specs=(
            P(None, "row", "seq"),
            P(None, "col", "seq"),
            P("seq", "col"),
            P("seq", "row"),
            P(),
        ),
        out_specs=P(("row", "seq"), "col"),
        check_vma=False,
    )
```

```python
import functools

import jax
import jax.numpy as jnp
from jax import lax
from jax.experimental import pallas as pl
from jax.experimental.pallas import tpu as pltpu
from jax.sharding import PartitionSpec as P

MESH = pl.DeviceIdType.MESH
F32 = jnp.float32
BF16 = jnp.bfloat16

PHASES = dict(rs1_in=6, rs1_out=6, rs2_in=3, rs2_out=3, row=3, ag1=4, ag2=4, z=3, fwd=4, last=1)
FIRST = {}
TOTAL = 0
for _name, _count in PHASES.items():
    FIRST[_name] = TOTAL
    TOTAL += _count


def kernel(
    act_hbm, grad_hbm, bin_hbm, bout_hbm, len_ref, out_ref,
    act, grad, bin_, bout,
    p32_in, p16_in, p32_out, p16_out,
    got_in, got_out, tmp_in, tmp_out,
    q_in, q_out, got2_in, got2_out,
    t_in, gbuf, obuf, lhs, acc, xch,
    load_sem, send_sem, recv_sem,
):
    s = lax.axis_index("seq")
    r = lax.axis_index("row")
    c = lax.axis_index("col")
    y, x = lax.div(s, 4), lax.rem(s, 4)
    zl, k = lax.div(r, 2), lax.rem(r, 2)
    a = x + k * (y - x)
    b = y + k * (x - y)
    step_a, step_b = 1 + 3 * k, 4 - 3 * k

    def turn(v):
        return lax.rem(v + 4, 4)

    def at(a_, b_):
        return a_ * step_a + b_ * step_b

    def send(name, i, src, dst, device):
        n = FIRST[name] + i
        copy = pltpu.make_async_remote_copy(
            src_ref=src, dst_ref=dst, send_sem=send_sem.at[n], recv_sem=recv_sem.at[n],
            device_id=device, device_id_type=MESH,
        )
        copy.start()
        return copy

    loads = [
        pltpu.make_async_copy(src, dst, load_sem.at[i])
        for i, (src, dst) in enumerate(
            [(act_hbm, act), (bin_hbm, bin_), (grad_hbm, grad), (bout_hbm, bout)]
        )
    ]
    for load in loads:
        load.start()

    barrier = pltpu.get_barrier_semaphore()
    peers = []
    for d in (1, 2, 3):
        peers.append((at(turn(a + d), b), r, c))
        peers.append((at(a, turn(b + d)), r, c))
        peers.append((s, lax.rem(r + d, 4), c))
        peers.append((s, r, lax.rem(c + d, 4)))
    for peer in peers:
        pl.semaphore_signal(barrier, inc=1, device_id=peer, device_id_type=MESH)

    ap, am, a2 = turn(a + 1), turn(a - 1), turn(a + 2)
    bp, bm, b2 = turn(b + 1), turn(b - 1), turn(b + 2)
    right, left = (at(ap, b), r, c), (at(am, b), r, c)

    loads[0].wait()
    loads[1].wait()
    for j in range(4):
        m = jnp.dot(act[...], bin_[:, 256 * j : 256 * (j + 1)], preferred_element_type=F32)
        for i in range(4):
            blk = m[64 * i : 64 * (i + 1)]
            at_blk = i * step_a + j * step_b
            p32_in[at_blk] = blk
            p16_in[at_blk] = blk.astype(BF16)

    pl.semaphore_wait(barrier, len(peers))

    def ring1_start(name, p16, got):
        return [
            send(name, 0, p16.at[pl.ds(a2 * 4, 2)], got.at[0], right),
            send(name, 1, p16.at[pl.ds(a2 * 4 + 2, 2)], got.at[1], left),
            send(name, 2, p16.at[pl.ds(ap * 4 + 2, 2)], got.at[2], right),
            send(name, 3, p16.at[pl.ds(am * 4, 2)], got.at[3], left),
        ]

    def ring1_relay(name, copies, p32, got, tmp):
        copies[0].wait_recv()
        tmp[0] = (got[0].astype(F32) + p32[pl.ds(ap * 4, 2)]).astype(BF16)
        copies.append(send(name, 4, tmp.at[0], got.at[4], right))
        copies[1].wait_recv()
        tmp[1] = (got[1].astype(F32) + p32[pl.ds(am * 4 + 2, 2)]).astype(BF16)
        copies.append(send(name, 5, tmp.at[1], got.at[5], left))

    def ring1_end(copies, p32, got, q):
        copies[2].wait_recv()
        copies[3].wait_recv()
        copies[4].wait_recv()
        copies[5].wait_recv()
        q[0:2] = p32[pl.ds(a * 4, 2)] + got[3].astype(F32) + got[4].astype(F32)
        q[2:4] = p32[pl.ds(a * 4 + 2, 2)] + got[2].astype(F32) + got[5].astype(F32)

    def ring2_start(name, q, got2):
        return [
            send(name, d - 1, q.at[turn(b + d)], got2.at[d - 1], (at(a, turn(b + d)), r, c))
            for d in (2, 1, 3)
        ]

    def ring2_end(copies, q, got2):
        for copy in copies:
            copy.wait_recv()
        return q[b] + got2[0] + got2[1] + got2[2]

    pending = []
    rs1_in = ring1_start("rs1_in", p16_in, got_in)

    loads[2].wait()
    loads[3].wait()
    for j in range(4):
        m = jnp.dot(grad[...], bout[:, 256 * j : 256 * (j + 1)], preferred_element_type=F32)
        m = m.T
        for i in range(4):
            blk = m[64 * i : 64 * (i + 1)]
            at_blk = i * step_b + j * step_a
            p32_out[at_blk] = blk
            p16_out[at_blk] = blk.astype(BF16)
    rs1_out = ring1_start("rs1_out", p16_out, got_out)

    ring1_relay("rs1_in", rs1_in, p32_in, got_in, tmp_in)
    ring1_relay("rs1_out", rs1_out, p32_out, got_out, tmp_out)

    ring1_end(rs1_in, p32_in, got_in, q_in)
    rs2_in = ring2_start("rs2_in", q_in, got2_in)
    ring1_end(rs1_out, p32_out, got_out, q_out)
    rs2_out = ring2_start("rs2_out", q_out, got2_out)

    turned = ring2_end(rs2_in, q_in, got2_in).astype(BF16)
    t_in[0] = turned[:, :128]
    t_in[1] = turned[:, 128:]
    gbuf[a, b, r] = t_in[k]
    row = [
        send("row", 0, t_in.at[1 - k], gbuf.at[b, a, r], (s, 2 * zl + 1 - k, c)),
        send("row", 1, t_in.at[k], gbuf.at[a, b, r], (s, 2 * (1 - zl) + k, c)),
        send("row", 2, t_in.at[1 - k], gbuf.at[b, a, r], (s, 2 * (1 - zl) + 1 - k, c)),
    ]

    obuf[k, c] = ring2_end(rs2_out, q_out, got2_out).astype(BF16)
    partner = (s, 2 * zl + 1 - k, c)
    z = [
        send("z", d - 1, obuf.at[k, c], obuf.at[k, c], (s, r, turn(c + d)))
        for d in (2, 1, 3)
    ]
    fwd = [send("fwd", 0, obuf.at[k, c], obuf.at[k, c], partner)]

    for copy in row:
        copy.wait_recv()
    right_b, left_b = (at(a, bp), r, c), (at(a, bm), r, c)
    ag1 = [
        send("ag1", 0, gbuf.at[a, b], gbuf.at[a, b], right_b),
        send("ag1", 1, gbuf.at[a, b], gbuf.at[a, b], left_b),
    ]
    ag1[0].wait_recv()
    ag1.append(send("ag1", 2, gbuf.at[a, bm, pl.ds(0, 2)], gbuf.at[a, bm, pl.ds(0, 2)], right_b))
    ag1[1].wait_recv()
    ag1.append(send("ag1", 3, gbuf.at[a, bp, pl.ds(2, 2)], gbuf.at[a, bp, pl.ds(2, 2)], left_b))
    ag1[2].wait_recv()
    ag1[3].wait_recv()
    ag2 = [
        send("ag2", 0, gbuf.at[a], gbuf.at[a], right),
        send("ag2", 1, gbuf.at[a], gbuf.at[a], left),
    ]

    for i, d in enumerate((2, 1, 3)):
        z[i].wait_recv()
        from_ = turn(c - d)
        fwd.append(send("fwd", i + 1, obuf.at[k, from_], obuf.at[k, from_], partner))
    for copy in fwd:
        copy.wait_recv()

    lane = lax.broadcasted_iota(jnp.int32, (64, 256), 1)
    seq4 = lax.rem(lax.div(lane, 16), 4)
    slot = lax.div(lane, 64) * 16 + lax.rem(lane, 16)
    for g in range(4):
        keep = [
            jnp.logical_and(seq4 == i, slot < len_ref[4 * g + i]) for i in range(4)
        ]
        for kk in range(2):
            whole = jnp.concatenate(
                [obuf[kk, zz].astype(F32)[:, 64 * g : 64 * (g + 1)] for zz in range(4)], axis=1
            )
            for i in range(4):
                lhs[g, kk, i] = jnp.where(keep[i], whole, 0.0).astype(BF16)

    acc[...] = jnp.zeros_like(acc)

    def use(a_):
        for b_ in range(4):
            gy = b_ + k * (a_ - b_)
            gx = a_ + k * (b_ - a_)
            prod = jnp.dot(
                lhs[gy].reshape(512, 256), gbuf[a_, b_].reshape(256, 128),
                preferred_element_type=F32,
            )
            acc[:, gx] += jnp.sum((prod * prod).reshape(2, 4, 64, 128), axis=1)

    use(a)
    ag2[0].wait_recv()
    ag2.append(send("ag2", 2, gbuf.at[am, pl.ds(0, 2)], gbuf.at[am, pl.ds(0, 2)], right))
    ag2[1].wait_recv()
    ag2.append(send("ag2", 3, gbuf.at[ap, pl.ds(2, 2)], gbuf.at[ap, pl.ds(2, 2)], left))
    use(am)
    use(ap)
    ag2[2].wait_recv()
    ag2[3].wait_recv()
    use(a2)

    acc[...] = acc[...] * (1.0 / 1024.0)
    last = [send("last", 0, acc.at[1 - k], xch, partner)]
    for g in range(4):
        out_ref[:, pl.ds(pl.multiple_of(g * 256 + k * 128, 128), 128)] = acc[k, g]
    last[0].wait_recv()
    for g in range(4):
        out_ref[:, pl.ds(pl.multiple_of(g * 256 + (1 - k) * 128, 128), 128)] = xch[g]

    for copies in (rs1_in, rs1_out, rs2_in, rs2_out, row, z, fwd, ag1, ag2, last):
        for copy in copies:
            copy.wait_send()


def local(activations, gradients, basis_in, basis_out, lengths):
    any_ = pl.BlockSpec(memory_space=pl.ANY)
    vm = pltpu.VMEM
    return pl.pallas_call(
        kernel,
        out_shape=jax.ShapeDtypeStruct((64, 1024), F32),
        in_specs=[any_] * 4 + [pl.BlockSpec(memory_space=pltpu.SMEM)],
        out_specs=pl.BlockSpec(memory_space=pltpu.VMEM),
        scratch_shapes=[
            vm((256, 512), BF16), vm((256, 512), BF16),
            vm((512, 1024), BF16), vm((512, 1024), BF16),
            vm((16, 64, 256), F32), vm((16, 64, 256), BF16),
            vm((16, 64, 256), F32), vm((16, 64, 256), BF16),
            vm((6, 2, 64, 256), BF16), vm((6, 2, 64, 256), BF16),
            vm((2, 2, 64, 256), BF16), vm((2, 2, 64, 256), BF16),
            vm((4, 64, 256), F32), vm((4, 64, 256), F32),
            vm((3, 64, 256), F32), vm((3, 64, 256), F32),
            vm((2, 64, 128), BF16),
            vm((4, 4, 4, 64, 128), BF16),
            vm((2, 4, 64, 256), BF16),
            vm((4, 2, 4, 64, 256), BF16),
            vm((2, 4, 64, 128), F32),
            vm((4, 64, 128), F32),
            pltpu.SemaphoreType.DMA((4,)),
            pltpu.SemaphoreType.DMA((TOTAL,)),
            pltpu.SemaphoreType.DMA((TOTAL,)),
        ],
        compiler_params=pltpu.CompilerParams(
            collective_id=0, has_side_effects=True, vmem_limit_bytes=60 * 1024 * 1024
        ),
    )(
        activations.reshape(256, 512), gradients.reshape(256, 512),
        basis_in, basis_out, lengths,
    )


def solution(mesh):
    return jax.shard_map(
        local,
        mesh=mesh,
        in_specs=(
            P(None, "row", "seq"),
            P(None, "col", "seq"),
            P("seq", "col"),
            P("seq", "row"),
            P(),
        ),
        out_specs=P(("row", "seq"), "col"),
        check_vma=False,
    )
```

```python
import jax
import jax.numpy as jnp
from jax import lax
from jax.experimental import pallas as pl
from jax.experimental.pallas import tpu as pltpu
from jax.sharding import PartitionSpec as P

MESH = pl.DeviceIdType.MESH
F32 = jnp.float32
BF16 = jnp.bfloat16

PHASES = dict(
    rs1_in=6, rs1_out=6, rs2_in=7, rs2_out=3, zx=1, ag1=6, ag2=32, z=3, fwd=4, last=4
)
FIRST = {}
TOTAL = 0
for _name, _count in PHASES.items():
    FIRST[_name] = TOTAL
    TOTAL += _count


def kernel(
    act_hbm, grad_hbm, bin_hbm, bout_hbm, len_ref, out_ref,
    act, grad, bin_, bout,
    p32_in, p16_in, p32_out, p16_out,
    got_in, got_out, tmp_in, tmp_out,
    q_in, q_out, same, cross, got2_out,
    gbuf, obuf, lhs, acc, xch,
    load_sem, send_sem, recv_sem,
):
    s = lax.axis_index("seq")
    r = lax.axis_index("row")
    c = lax.axis_index("col")
    y, x = lax.div(s, 4), lax.rem(s, 4)
    zl, k = lax.div(r, 2), lax.rem(r, 2)
    a = x + k * (y - x)
    b = y + k * (x - y)
    step_a, step_b = 1 + 3 * k, 4 - 3 * k

    def turn(v):
        return lax.rem(v + 4, 4)

    def at(a_, b_):
        return a_ * step_a + b_ * step_b

    started = []

    def send(name, i, src, dst, device):
        n = FIRST[name] + i
        copy = pltpu.make_async_remote_copy(
            src_ref=src, dst_ref=dst, send_sem=send_sem.at[n], recv_sem=recv_sem.at[n],
            device_id=device, device_id_type=MESH,
        )
        copy.start()
        started.append(copy)
        return copy

    loads = [
        pltpu.make_async_copy(src, dst, load_sem.at[i])
        for i, (src, dst) in enumerate(
            [(act_hbm, act), (bin_hbm, bin_), (grad_hbm, grad), (bout_hbm, bout)]
        )
    ]
    for load in loads:
        load.start()

    ap, am, a2 = turn(a + 1), turn(a - 1), turn(a + 2)
    other = 2 * zl + 1 - k
    partner = (s, other, c)
    right, left = (at(ap, b), r, c), (at(am, b), r, c)
    across = (s, 2 * (1 - zl) + k, c)

    barrier = pltpu.get_barrier_semaphore()
    peers = [right, left, partner, across]
    for d in (1, 2, 3):
        peers.append((at(a, turn(b + d)), r, c))
        peers.append((at(a, turn(b + d)), other, c))
        peers.append((at(turn(a + d), b), other, c))
        peers.append((s, r, turn(c + d)))
    for peer in peers:
        pl.semaphore_signal(barrier, inc=1, device_id=peer, device_id_type=MESH)

    loads[0].wait()
    loads[1].wait()
    for j in range(4):
        m = jnp.dot(act[...], bin_[:, 256 * j : 256 * (j + 1)], preferred_element_type=F32)
        for h in range(2):
            sc = h + k - 2 * h * k
            for i in range(4):
                blk = m[64 * i : 64 * (i + 1), 128 * h : 128 * (h + 1)]
                at_blk = 4 * j + i + 3 * (i - j) * sc
                p32_in[at_blk, sc] = blk
                p16_in[at_blk, sc] = blk.astype(BF16)

    pl.semaphore_wait(barrier, len(peers))

    def ring1_start(name, p16, got):
        return [
            send(name, 0, p16.at[pl.ds(a2 * 4, 2)], got.at[0], right),
            send(name, 1, p16.at[pl.ds(a2 * 4 + 2, 2)], got.at[1], left),
            send(name, 2, p16.at[pl.ds(ap * 4 + 2, 2)], got.at[2], right),
            send(name, 3, p16.at[pl.ds(am * 4, 2)], got.at[3], left),
        ]

    def ring1_relay(name, copies, p32, got, tmp):
        copies[0].wait_recv()
        tmp[0] = (got[0].astype(F32) + p32[pl.ds(ap * 4, 2)]).astype(BF16)
        copies.append(send(name, 4, tmp.at[0], got.at[4], right))
        copies[1].wait_recv()
        tmp[1] = (got[1].astype(F32) + p32[pl.ds(am * 4 + 2, 2)]).astype(BF16)
        copies.append(send(name, 5, tmp.at[1], got.at[5], left))

    def ring1_end(copies, p32, got, q):
        copies[2].wait_recv()
        copies[3].wait_recv()
        copies[4].wait_recv()
        q[0:2] = p32[pl.ds(a * 4, 2)] + got[3].astype(F32) + got[4].astype(F32)
        copies[5].wait_recv()
        q[2:4] = p32[pl.ds(a * 4 + 2, 2)] + got[2].astype(F32) + got[5].astype(F32)

    rs1_in = ring1_start("rs1_in", p16_in, got_in)

    loads[2].wait()
    loads[3].wait()
    for j in range(4):
        m = jnp.dot(grad[...], bout[:, 256 * j : 256 * (j + 1)], preferred_element_type=F32)
        m = m.T
        for i in range(4):
            blk = m[64 * i : 64 * (i + 1)]
            at_blk = 4 * i + j + 3 * (j - i) * k
            p32_out[at_blk] = blk
            p16_out[at_blk] = blk.astype(BF16)
    rs1_out = ring1_start("rs1_out", p16_out, got_out)

    ring1_relay("rs1_in", rs1_in, p32_in, got_in, tmp_in)
    ring1_relay("rs1_out", rs1_out, p32_out, got_out, tmp_out)

    ring1_end(rs1_in, p32_in, got_in, q_in)
    rs2_same, rs2_cross = [], []
    for d in (2, 1, 3):
        to = turn(b + d)
        rs2_same.append(
            send("rs2_in", d - 1, q_in.at[to, 0], same.at[d - 1], (at(a, to), r, c))
        )
        rs2_cross.append(
            send("rs2_in", 3 + d, q_in.at[to, 1], cross.at[d], (at(a, to), other, c))
        )
    rs2_cross.append(send("rs2_in", 3, q_in.at[b, 1], cross.at[0], partner))

    ring1_end(rs1_out, p32_out, got_out, q_out)
    rs2_out = [
        send("rs2_out", d - 1, q_out.at[turn(b + d)], got2_out.at[d - 1], (at(a, turn(b + d)), r, c))
        for d in (2, 1, 3)
    ]

    for copy in rs2_same + rs2_cross:
        copy.wait_recv()
    gbuf[a, b, zl, k] = (q_in[b, 0] + same[0] + same[1] + same[2]).astype(BF16)
    gbuf[a, b, zl, 1 - k] = (cross[0] + cross[1] + cross[2] + cross[3]).astype(BF16)

    def unit(a_, b_, w):
        return gbuf.at[a_, b_, w]

    def along_b(wi, w):
        return {
            d: send("ag1", 3 * wi + d - 1, unit(a, b, w), unit(a, b, w), (at(a, turn(b + d)), r, c))
            for d in (2, 1, 3)
        }

    def along_a(bi, wi, w):
        b_ = turn(b + bi)
        n = 4 * (4 * wi + bi)
        return [
            send("ag2", n, unit(a, b_, w), unit(a, b_, w), right),
            send("ag2", n + 1, unit(a, b_, w), unit(a, b_, w), left),
        ]

    def pass_on(copies, bi, wi, w):
        b_ = turn(b + bi)
        n = 4 * (4 * wi + bi)
        copies[0].wait_recv()
        copies.append(send("ag2", n + 2, gbuf.at[am, b_, w, 0], gbuf.at[am, b_, w, 0], right))
        copies[1].wait_recv()
        copies.append(send("ag2", n + 3, gbuf.at[ap, b_, w, 1], gbuf.at[ap, b_, w, 1], left))

    w0, w1 = zl, 1 - zl
    ring_a = {}
    zx = send("zx", 0, unit(a, b, w0), unit(a, b, w0), across)
    ring_b0 = along_b(0, w0)
    ring_a[0, 0] = along_a(0, 0, w0)

    for copy in rs2_out:
        copy.wait_recv()
    obuf[k, c] = (q_out[b] + got2_out[0] + got2_out[1] + got2_out[2]).astype(BF16)
    z = [
        send("z", d - 1, obuf.at[k, c], obuf.at[k, c], (s, r, turn(c + d)))
        for d in (2, 1, 3)
    ]
    fwd = [send("fwd", 0, obuf.at[k, c], obuf.at[k, c], partner)]

    zx.wait_recv()
    ring_b1 = along_b(1, w1)
    ring_a[0, 1] = along_a(0, 1, w1)
    for d in (1, 3):
        ring_b0[d].wait_recv()
        ring_a[4 - d, 0] = along_a(4 - d, 0, w0)
    pass_on(ring_a[0, 0], 0, 0, w0)
    ring_b0[2].wait_recv()
    ring_a[2, 0] = along_a(2, 0, w0)
    for d in (1, 3):
        ring_b1[d].wait_recv()
        ring_a[4 - d, 1] = along_a(4 - d, 1, w1)
    pass_on(ring_a[0, 1], 0, 1, w1)
    pass_on(ring_a[3, 0], 3, 0, w0)
    pass_on(ring_a[1, 0], 1, 0, w0)
    ring_b1[2].wait_recv()
    ring_a[2, 1] = along_a(2, 1, w1)

    for i, d in enumerate((2, 1, 3)):
        z[i].wait_recv()
        from_ = turn(c - d)
        fwd.append(send("fwd", i + 1, obuf.at[k, from_], obuf.at[k, from_], partner))
    pass_on(ring_a[2, 0], 2, 0, w0)
    pass_on(ring_a[3, 1], 3, 1, w1)
    pass_on(ring_a[1, 1], 1, 1, w1)
    for copy in fwd:
        copy.wait_recv()

    lane = lax.broadcasted_iota(jnp.int32, (64, 256), 1)
    seq4 = lax.rem(lax.div(lane, 16), 4)
    slot = lax.div(lane, 64) * 16 + lax.rem(lane, 16)
    for g in range(4):
        keep = [
            jnp.logical_and(seq4 == i, slot < len_ref[4 * g + i]) for i in range(4)
        ]
        for kk in range(2):
            whole = jnp.concatenate(
                [obuf[kk, zz].astype(F32)[:, 64 * g : 64 * (g + 1)] for zz in range(4)], axis=1
            )
            for i in range(4):
                lhs[g, kk, i] = jnp.where(keep[i], whole, 0.0).astype(BF16)
    pass_on(ring_a[2, 1], 2, 1, w1)

    last = []

    def use(i, a_):
        total = jnp.zeros((2, 64, 128), F32)
        for g in range(4):
            prod = jnp.dot(
                lhs[g].reshape(512, 256), gbuf[a_, g].reshape(256, 128),
                preferred_element_type=F32,
            )
            total += jnp.sum((prod * prod).reshape(2, 4, 64, 128), axis=1)
        acc[i] = total * (1.0 / 1024.0)
        last.append(send("last", i, acc.at[i, 1 - k], xch.at[i], partner))
        out_ref[:, pl.ds(pl.multiple_of(a_ * 256 + k * 128, 128), 128)] = acc[i, k]

    use(0, a)
    use(1, am)
    use(2, ap)
    for bi, wi in ((0, 0), (0, 1), (3, 0), (1, 0), (2, 0), (3, 1), (1, 1), (2, 1)):
        ring_a[bi, wi][2].wait_recv()
        ring_a[bi, wi][3].wait_recv()
    use(3, a2)

    for i, step in enumerate((0, 3, 1, 2)):
        last[i].wait_recv()
        at_col = turn(b + step) * 256 + (1 - k) * 128
        out_ref[:, pl.ds(pl.multiple_of(at_col, 128), 128)] = xch[i]

    for copy in started:
        copy.wait_send()


def local(activations, gradients, basis_in, basis_out, lengths):
    hbm = pl.BlockSpec(memory_space=pltpu.HBM)
    vm = pltpu.VMEM
    return pl.pallas_call(
        kernel,
        out_shape=jax.ShapeDtypeStruct((64, 1024), F32),
        in_specs=[hbm] * 4 + [pl.BlockSpec(memory_space=pltpu.SMEM)],
        out_specs=pl.BlockSpec(memory_space=pltpu.VMEM),
        scratch_shapes=[
            vm((256, 512), BF16), vm((256, 512), BF16),
            vm((512, 1024), BF16), vm((512, 1024), BF16),
            vm((16, 2, 64, 128), F32), vm((16, 2, 64, 128), BF16),
            vm((16, 64, 256), F32), vm((16, 64, 256), BF16),
            vm((6, 2, 2, 64, 128), BF16), vm((6, 2, 64, 256), BF16),
            vm((2, 2, 2, 64, 128), BF16), vm((2, 2, 64, 256), BF16),
            vm((4, 2, 64, 128), F32), vm((4, 64, 256), F32),
            vm((3, 64, 128), F32), vm((4, 64, 128), F32), vm((3, 64, 256), F32),
            vm((4, 4, 2, 2, 64, 128), BF16),
            vm((2, 4, 64, 256), BF16),
            vm((4, 2, 4, 64, 256), BF16),
            vm((4, 2, 64, 128), F32),
            vm((4, 64, 128), F32),
            pltpu.SemaphoreType.DMA((4,)),
            pltpu.SemaphoreType.DMA((TOTAL,)),
            pltpu.SemaphoreType.DMA((TOTAL,)),
        ],
        compiler_params=pltpu.CompilerParams(
            collective_id=0, has_side_effects=True, vmem_limit_bytes=40 * 1024 * 1024
        ),
    )(
        *[
            pltpu.with_memory_space_constraint(v, pltpu.HBM)
            for v in (
                activations.reshape(256, 512), gradients.reshape(256, 512), basis_in, basis_out
            )
        ],
        pltpu.with_memory_space_constraint(lengths, pltpu.HBM),
    )


def solution(mesh):
    return jax.shard_map(
        local,
        mesh=mesh,
        in_specs=(
            P(None, "row", "seq"),
            P(None, "col", "seq"),
            P("seq", "col"),
            P("seq", "row"),
            P(),
        ),
        out_specs=P(("row", "seq"), "col"),
        check_vma=False,
    )
```

```python
import jax
import jax.numpy as jnp
from jax import lax
from jax.experimental import pallas as pl
from jax.experimental.pallas import tpu as pltpu
from jax.sharding import PartitionSpec as P

MESH = pl.DeviceIdType.MESH
F32 = jnp.float32
BF16 = jnp.bfloat16

PHASES = dict(
    rs1_in=3, rs1_out=3, rs2_in=7, rs2_out=3, ag1=7, ag2=24, z=3, fwd=4, last=4
)
FIRST = {}
TOTAL = 0
for _name, _count in PHASES.items():
    FIRST[_name] = TOTAL
    TOTAL += _count


def kernel(
    act_hbm, grad_hbm, bin_hbm, bout_hbm, len_ref, out_ref,
    act, grad, bin_, bout,
    p32_in, p16_in, p32_out, p16_out,
    got_in, got_out,
    q_in, q_out, same, cross, got2_out,
    gbuf, obuf, lhs, acc, xch,
    load_sem, send_sem, recv_sem,
):
    s = lax.axis_index("seq")
    r = lax.axis_index("row")
    c = lax.axis_index("col")
    y, x = lax.div(s, 4), lax.rem(s, 4)
    zl, k = lax.div(r, 2), lax.rem(r, 2)
    a = x + k * (y - x)
    b = y + k * (x - y)
    step_a, step_b = 1 + 3 * k, 4 - 3 * k

    def turn(v):
        return lax.rem(v + 4, 4)

    def at(a_, b_):
        return a_ * step_a + b_ * step_b

    started = []

    def send(name, i, src, dst, device):
        n = FIRST[name] + i
        copy = pltpu.make_async_remote_copy(
            src_ref=src, dst_ref=dst, send_sem=send_sem.at[n], recv_sem=recv_sem.at[n],
            device_id=device, device_id_type=MESH,
        )
        copy.start()
        started.append(copy)
        return copy

    loads = [
        pltpu.make_async_copy(src, dst, load_sem.at[i])
        for i, (src, dst) in enumerate(
            [(act_hbm, act), (bin_hbm, bin_), (grad_hbm, grad), (bout_hbm, bout)]
        )
    ]
    for load in loads:
        load.start()

    ap, am, a2 = turn(a + 1), turn(a - 1), turn(a + 2)
    bp, bm, b2 = turn(b + 1), turn(b - 1), turn(b + 2)
    other = 2 * zl + 1 - k
    partner = (s, other, c)
    right, left = (at(ap, b), r, c), (at(am, b), r, c)
    over = 2 * (1 - zl) + k
    far = (at(a2, b), r, c)

    barrier = pltpu.get_barrier_semaphore()
    peers = [right, left, far, partner, (s, over, c)]
    for d in (1, 2, 3):
        peers.append((at(a, turn(b + d)), r, c))
        peers.append((at(a, turn(b + d)), other, c))
        peers.append((at(a, turn(b + d)), over, c))
        peers.append((at(turn(a + d), b), other, c))
        peers.append((s, r, turn(c + d)))
    for peer in peers:
        pl.semaphore_signal(barrier, inc=1, device_id=peer, device_id_type=MESH)

    loads[0].wait()
    loads[1].wait()
    for j in range(4):
        m = jnp.dot(act[...], bin_[:, 256 * j : 256 * (j + 1)], preferred_element_type=F32)
        for h in range(2):
            sc = h + k - 2 * h * k
            for i in range(4):
                blk = m[64 * i : 64 * (i + 1), 128 * h : 128 * (h + 1)]
                at_blk = 4 * j + i + 3 * (i - j) * sc
                p32_in[at_blk, sc] = blk
                p16_in[at_blk, sc] = blk.astype(BF16)

    pl.semaphore_wait(barrier, len(peers))

    def ring1_start(name, p16, got):
        return [
            send(name, d - 1, p16.at[pl.ds(turn(a + d) * 4, 4)], got.at[d - 1], to)
            for d, to in ((2, far), (1, right), (3, left))
        ]

    def ring1_end(copies, p32, got, q):
        for copy in copies:
            copy.wait_recv()
        q[...] = (
            p32[pl.ds(a * 4, 4)]
            + got[0].astype(F32) + got[1].astype(F32) + got[2].astype(F32)
        )

    rs1_in = ring1_start("rs1_in", p16_in, got_in)

    loads[2].wait()
    loads[3].wait()
    for j in range(4):
        m = jnp.dot(grad[...], bout[:, 256 * j : 256 * (j + 1)], preferred_element_type=F32)
        m = m.T
        for i in range(4):
            blk = m[64 * i : 64 * (i + 1)]
            at_blk = 4 * i + j + 3 * (j - i) * k
            p32_out[at_blk] = blk
            p16_out[at_blk] = blk.astype(BF16)
    rs1_out = ring1_start("rs1_out", p16_out, got_out)

    ring1_end(rs1_in, p32_in, got_in, q_in)
    rs2_same, rs2_cross = [], []
    for d in (2, 1, 3):
        to = turn(b + d)
        rs2_same.append(
            send("rs2_in", d - 1, q_in.at[to, 0], same.at[d - 1], (at(a, to), r, c))
        )
        rs2_cross.append(
            send("rs2_in", 3 + d, q_in.at[to, 1], cross.at[d], (at(a, to), other, c))
        )
    rs2_cross.append(send("rs2_in", 3, q_in.at[b, 1], cross.at[0], partner))

    ring1_end(rs1_out, p32_out, got_out, q_out)
    rs2_out = [
        send("rs2_out", d - 1, q_out.at[turn(b + d)], got2_out.at[d - 1], (at(a, turn(b + d)), r, c))
        for d in (2, 1, 3)
    ]

    for copy in rs2_same + rs2_cross:
        copy.wait_recv()
    gbuf[a, b, zl, k] = (q_in[b, 0] + same[0] + same[1] + same[2]).astype(BF16)
    gbuf[a, b, zl, 1 - k] = (cross[0] + cross[1] + cross[2] + cross[3]).astype(BF16)

    def unit(a_, b_, w):
        return gbuf.at[a_, b_, w]

    def own_to(n, b_, row):
        return send("ag1", n, unit(a, b, w0), unit(a, b, w0), (at(a, b_), row, c))

    def along_a(bi, wi):
        b_, w = turn(b + bi), (w0, w1)[wi]
        for d, to in ((2, far), (1, right), (3, left)):
            n = 3 * (4 * wi + bi) + d - 1
            ring_a[bi, wi, d] = send("ag2", n, unit(a, b_, w), unit(a, b_, w), to)

    w0, w1 = zl, 1 - zl
    ring_a = {}
    along_a(0, 0)
    near, away = {}, {}
    near[2] = own_to(1, b2, r)
    away[0] = own_to(3, b, over)
    away[2] = own_to(5, b2, over)
    near[1] = own_to(0, bp, r)
    near[3] = own_to(2, bm, r)
    away[1] = own_to(4, bp, over)
    away[3] = own_to(6, bm, over)

    for copy in rs2_out:
        copy.wait_recv()
    obuf[k, c] = (q_out[b] + got2_out[0] + got2_out[1] + got2_out[2]).astype(BF16)
    z = [
        send("z", d - 1, obuf.at[k, c], obuf.at[k, c], (s, r, turn(c + d)))
        for d in (2, 1, 3)
    ]
    fwd = [send("fwd", 0, obuf.at[k, c], obuf.at[k, c], partner)]

    away[0].wait_recv()
    along_a(0, 1)
    for d in (1, 3):
        near[d].wait_recv()
        along_a(4 - d, 0)
    for d in (1, 3):
        away[d].wait_recv()
        along_a(4 - d, 1)
    near[2].wait_recv()
    along_a(2, 0)
    away[2].wait_recv()
    along_a(2, 1)

    for i, d in enumerate((2, 1, 3)):
        z[i].wait_recv()
        from_ = turn(c - d)
        fwd.append(send("fwd", i + 1, obuf.at[k, from_], obuf.at[k, from_], partner))
    for copy in fwd:
        copy.wait_recv()

    lane = lax.broadcasted_iota(jnp.int32, (64, 256), 1)
    seq4 = lax.rem(lax.div(lane, 16), 4)
    slot = lax.div(lane, 64) * 16 + lax.rem(lane, 16)
    for g in range(4):
        keep = [
            jnp.logical_and(seq4 == i, slot < len_ref[4 * g + i]) for i in range(4)
        ]
        for kk in range(2):
            whole = jnp.concatenate(
                [obuf[kk, zz].astype(F32)[:, 64 * g : 64 * (g + 1)] for zz in range(4)], axis=1
            )
            for i in range(4):
                lhs[g, kk, i] = jnp.where(keep[i], whole, 0.0).astype(BF16)

    last = []

    def use(i, a_):
        total = jnp.zeros((2, 64, 128), F32)
        for g in range(4):
            prod = jnp.dot(
                lhs[g].reshape(512, 256), gbuf[a_, g].reshape(256, 128),
                preferred_element_type=F32,
            )
            total += jnp.sum((prod * prod).reshape(2, 4, 64, 128), axis=1)
        acc[i] = total * (1.0 / 1024.0)
        last.append(send("last", i, acc.at[i, 1 - k], xch.at[i], partner))
        out_ref[:, pl.ds(pl.multiple_of(a_ * 256 + k * 128, 128), 128)] = acc[i, k]

    use(0, a)
    for i, d, a_ in ((1, 1, am), (2, 3, ap), (3, 2, a2)):
        for wi in range(2):
            for bi in range(4):
                ring_a[bi, wi, d].wait_recv()
        use(i, a_)

    for i, step in enumerate((0, 3, 1, 2)):
        last[i].wait_recv()
        at_col = turn(b + step) * 256 + (1 - k) * 128
        out_ref[:, pl.ds(pl.multiple_of(at_col, 128), 128)] = xch[i]

    for copy in started:
        copy.wait_send()


def local(activations, gradients, basis_in, basis_out, lengths):
    hbm = pl.BlockSpec(memory_space=pltpu.HBM)
    vm = pltpu.VMEM
    return pl.pallas_call(
        kernel,
        out_shape=jax.ShapeDtypeStruct((64, 1024), F32),
        in_specs=[hbm] * 4 + [pl.BlockSpec(memory_space=pltpu.SMEM)],
        out_specs=pl.BlockSpec(memory_space=pltpu.VMEM),
        scratch_shapes=[
            vm((256, 512), BF16), vm((256, 512), BF16),
            vm((512, 1024), BF16), vm((512, 1024), BF16),
            vm((16, 2, 64, 128), F32), vm((16, 2, 64, 128), BF16),
            vm((16, 64, 256), F32), vm((16, 64, 256), BF16),
            vm((3, 4, 2, 64, 128), BF16), vm((3, 4, 64, 256), BF16),
            vm((4, 2, 64, 128), F32), vm((4, 64, 256), F32),
            vm((3, 64, 128), F32), vm((4, 64, 128), F32), vm((3, 64, 256), F32),
            vm((4, 4, 2, 2, 64, 128), BF16),
            vm((2, 4, 64, 256), BF16),
            vm((4, 2, 4, 64, 256), BF16),
            vm((4, 2, 64, 128), F32),
            vm((4, 64, 128), F32),
            pltpu.SemaphoreType.DMA((4,)),
            pltpu.SemaphoreType.DMA((TOTAL,)),
            pltpu.SemaphoreType.DMA((TOTAL,)),
        ],
        compiler_params=pltpu.CompilerParams(
            collective_id=0, has_side_effects=True, vmem_limit_bytes=40 * 1024 * 1024
        ),
    )(
        *[
            pltpu.with_memory_space_constraint(v, pltpu.HBM)
            for v in (
                activations.reshape(256, 512), gradients.reshape(256, 512), basis_in, basis_out
            )
        ],
        pltpu.with_memory_space_constraint(lengths, pltpu.HBM),
    )


def solution(mesh):
    return jax.shard_map(
        local,
        mesh=mesh,
        in_specs=(
            P(None, "row", "seq"),
            P(None, "col", "seq"),
            P("seq", "col"),
            P("seq", "row"),
            P(),
        ),
        out_specs=P(("row", "seq"), "col"),
        check_vma=False,
    )
```

```python
import jax
import jax.numpy as jnp
from jax import lax
from jax.experimental import pallas as pl
from jax.experimental.pallas import tpu as pltpu
from jax.sharding import PartitionSpec as P

MESH = pl.DeviceIdType.MESH
F32 = jnp.float32
BF16 = jnp.bfloat16

PHASES = dict(
    rs1_in=3, rs1_out=3, rs2_in=7, rs2_out=3, ag1=7, ag2=24, z=3, fw=13
)
FIRST = {}
TOTAL = 0
for _name, _count in PHASES.items():
    FIRST[_name] = TOTAL
    TOTAL += _count


def kernel(
    act_hbm, grad_hbm, bin_hbm, bout_hbm, len_ref, out_ref,
    act, grad, bin_, bout,
    p32_in, p16_in, p32_out, p16_out,
    got_in, got_out,
    q_in, q_out, q16_out, same, cross, got2_out,
    gbuf, obuf, lhs, acc,
    load_sem, send_sem, recv_sem, ready,
):
    s = lax.axis_index("seq")
    r = lax.axis_index("row")
    c = lax.axis_index("col")
    y, x = lax.div(s, 4), lax.rem(s, 4)
    zl, k = lax.div(r, 2), lax.rem(r, 2)
    a = x + k * (y - x)
    b = y + k * (x - y)
    step_a, step_b = 1 + 3 * k, 4 - 3 * k

    def turn(v):
        return lax.rem(v + 4, 4)

    def at(a_, b_):
        return a_ * step_a + b_ * step_b

    started = []

    def send(name, i, src, dst, device):
        n = FIRST[name] + i
        copy = pltpu.make_async_remote_copy(
            src_ref=src, dst_ref=dst, send_sem=send_sem.at[n], recv_sem=recv_sem.at[n],
            device_id=device, device_id_type=MESH,
        )
        copy.start()
        started.append(copy)
        return copy

    def load(i, src, dst):
        copy = pltpu.make_async_copy(src, dst, load_sem.at[i])
        copy.start()
        return copy

    load_act = load(0, act_hbm, act)
    load_bin = [
        load(1 + j, bin_hbm.at[:, pl.ds(256 * j, 256)], bin_.at[:, pl.ds(256 * j, 256)])
        for j in range(4)
    ]
    load_out = [load(5, grad_hbm, grad), load(6, bout_hbm, bout)]

    ap, am, a2 = turn(a + 1), turn(a - 1), turn(a + 2)
    bp, bm, b2 = turn(b + 1), turn(b - 1), turn(b + 2)
    other = 2 * zl + 1 - k
    partner = (s, other, c)
    right, left = (at(ap, b), r, c), (at(am, b), r, c)
    over = 2 * (1 - zl) + k
    far = (at(a2, b), r, c)

    barrier = pltpu.get_barrier_semaphore()

    def greet(s_, row_, c_):
        pl.semaphore_signal(barrier, inc=1, device_id=(s_, row_, c_), device_id_type=MESH)

    for d in (1, 2, 3):
        for s_ in (at(turn(a + d), b), at(a, turn(b + d))):
            greet(s_, 2 * zl, c)
            greet(s_, 2 * (1 - zl), c)
        greet(s, 2 * zl + 1, turn(c + d))
    greet(s, 2 * (1 - zl), c)

    @pl.when(k == 1)
    def _():
        greet(s, 2 * zl, c)

    load_act.wait()
    for j in range(4):
        load_bin[j].wait()
        m = jnp.dot(act[...], bin_[:, 256 * j : 256 * (j + 1)], preferred_element_type=F32)
        for h in range(2):
            sc = h + k - 2 * h * k
            for i in range(4):
                blk = m[64 * i : 64 * (i + 1), 128 * h : 128 * (h + 1)]
                at_blk = 4 * j + i + 3 * (i - j) * sc
                p32_in[at_blk, sc] = blk
                p16_in[at_blk, sc] = blk.astype(BF16)

    @pl.when(k == 0)
    def _():
        pl.semaphore_wait(barrier, 27)
        pl.semaphore_signal(ready, inc=1, device_id=partner, device_id_type=MESH)

    @pl.when(k == 1)
    def _():
        pl.semaphore_wait(ready, 1)

    def ring1_start(name, p16, got):
        return [
            send(name, d - 1, p16.at[pl.ds(turn(a + d) * 4, 4)], got.at[d - 1], to)
            for d, to in ((2, far), (1, right), (3, left))
        ]

    def ring1_end(copies, p32, got, q):
        for copy in copies:
            copy.wait_recv()
        q[...] = (
            p32[pl.ds(a * 4, 4)]
            + got[0].astype(F32) + got[1].astype(F32) + got[2].astype(F32)
        )

    rs1_in = ring1_start("rs1_in", p16_in, got_in)

    load_out[0].wait()
    load_out[1].wait()
    for j in range(4):
        m = jnp.dot(grad[...], bout[:, 256 * j : 256 * (j + 1)], preferred_element_type=F32)
        m = m.T
        for i in range(4):
            blk = m[64 * i : 64 * (i + 1)]
            at_blk = 4 * i + j + 3 * (j - i) * k
            p32_out[at_blk] = blk
            p16_out[at_blk] = blk.astype(BF16)
    rs1_out = ring1_start("rs1_out", p16_out, got_out)

    ring1_end(rs1_in, p32_in, got_in, q_in)
    rs2_same, rs2_cross = [], []
    for d in (2, 1, 3):
        to = turn(b + d)
        rs2_same.append(
            send("rs2_in", d - 1, q_in.at[to, 0], same.at[d - 1], (at(a, to), r, c))
        )
        rs2_cross.append(
            send("rs2_in", 3 + d, q_in.at[to, 1], cross.at[d], (at(a, to), other, c))
        )
    rs2_cross.append(send("rs2_in", 3, q_in.at[b, 1], cross.at[0], partner))

    ring1_end(rs1_out, p32_out, got_out, q_out)
    q16_out[...] = q_out[...].astype(BF16)
    rs2_out = [
        send("rs2_out", d - 1, q16_out.at[turn(b + d)], got2_out.at[d - 1], (at(a, turn(b + d)), r, c))
        for d in (2, 1, 3)
    ]

    for copy in rs2_same + rs2_cross:
        copy.wait_recv()
    gbuf[k, a, b, zl, k] = (q_in[b, 0] + same[0] + same[1] + same[2]).astype(BF16)
    gbuf[k, a, b, zl, 1 - k] = (cross[0] + cross[1] + cross[2] + cross[3]).astype(BF16)

    def unit(a_, b_, w):
        return gbuf.at[k, a_, b_, w]

    def own_to(n, b_, row):
        return send("ag1", n, unit(a, b, w0), unit(a, b, w0), (at(a, b_), row, c))

    def along_a(bi, wi):
        b_, w = turn(b + bi), (w0, w1)[wi]
        for d, to in ((2, far), (1, right), (3, left)):
            n = 3 * (4 * wi + bi) + d - 1
            ring_a[bi, wi, d] = send("ag2", n, unit(a, b_, w), unit(a, b_, w), to)

    w0, w1 = zl, 1 - zl
    ring_a = {}
    along_a(0, 0)
    near, away = {}, {}
    near[2] = own_to(1, b2, r)
    away[0] = own_to(3, b, over)
    away[2] = own_to(5, b2, over)
    near[1] = own_to(0, bp, r)
    near[3] = own_to(2, bm, r)
    away[1] = own_to(4, bp, over)
    away[3] = own_to(6, bm, over)

    for copy in rs2_out:
        copy.wait_recv()
    obuf[c] = (
        q_out[b] + got2_out[0].astype(F32) + got2_out[1].astype(F32) + got2_out[2].astype(F32)
    ).astype(BF16)

    @pl.when(k == 1)
    def _():
        pl.semaphore_wait(barrier, 6)
        pl.semaphore_signal(ready, inc=1, device_id=partner, device_id_type=MESH)

    @pl.when(k == 0)
    def _():
        pl.semaphore_wait(ready, 1)

    z = [
        send("z", d - 1, obuf.at[c], obuf.at[c], (s, r, turn(c + d)))
        for d in (2, 1, 3)
    ]

    away[0].wait_recv()
    along_a(0, 1)
    for d in (1, 3):
        near[d].wait_recv()
        along_a(4 - d, 0)
    for d in (1, 3):
        away[d].wait_recv()
        along_a(4 - d, 1)
    near[2].wait_recv()
    along_a(2, 0)
    away[2].wait_recv()
    along_a(2, 1)

    order = (0, 3, 1, 2)
    fw = {0: send("fw", 0, gbuf.at[k, a], gbuf.at[k, a], partner)}

    def forward(bi):
        b_ = turn(b + bi)
        for i, (d, a_) in enumerate(((1, am), (3, ap), (2, a2))):
            for wi in range(2):
                ring_a[bi, wi, d].wait_recv()
            n = 1 + 3 * bi + i
            fw[n] = send("fw", n, gbuf.at[k, a_, b_], gbuf.at[k, a_, b_], partner)

    for bi in order[:3]:
        forward(bi)
    for copy in z:
        copy.wait_recv()

    lane = lax.broadcasted_iota(jnp.int32, (64, 256), 1)
    seq4 = lax.rem(lax.div(lane, 16), 4)
    slot = lax.div(lane, 64) * 16 + lax.rem(lane, 16)
    outs = [obuf[zz].astype(F32) for zz in range(4)]
    for g in range(4):
        whole = jnp.concatenate([v[:, 64 * g : 64 * (g + 1)] for v in outs], axis=1)
        for i in range(4):
            keep = jnp.logical_and(seq4 == i, slot < len_ref[4 * g + i])
            lhs[g, i] = jnp.where(keep, whole, 0.0).astype(BF16)
    forward(order[3])

    acc[...] = jnp.zeros_like(acc)

    def use(part, half, g):
        left_side = lhs[g].reshape(256, 256)
        for pair in range(2):
            right_side = jnp.concatenate(
                [gbuf[half, 2 * pair + i, g].reshape(256, 128) for i in range(2)], axis=1
            )
            prod = jnp.dot(left_side, right_side, preferred_element_type=F32)
            prod = prod * prod
            acc[part, pair] += (prod[:64] + prod[64:128]) + (prod[128:192] + prod[192:])

    fw[0].wait_recv()
    for bi in order:
        use(0, k, turn(b + bi))
        for i in range(3):
            fw[1 + 3 * bi + i].wait_recv()
        use(1, 1 - k, turn(a + bi))

    for part, half in ((0, k), (1, 1 - k)):
        for g in range(4):
            at_col = pl.multiple_of(g * 256 + half * 128, 128)
            out_ref[:, pl.ds(at_col, 128)] = acc[
                part, g // 2, :, 128 * (g % 2) : 128 * (g % 2 + 1)
            ] * (1.0 / 1024.0)

    for copy in started:
        copy.wait_send()


def local(activations, gradients, basis_in, basis_out, lengths):
    hbm = pl.BlockSpec(memory_space=pltpu.HBM)
    vm = pltpu.VMEM
    return pl.pallas_call(
        kernel,
        out_shape=jax.ShapeDtypeStruct((64, 1024), F32),
        in_specs=[hbm] * 4 + [pl.BlockSpec(memory_space=pltpu.SMEM)],
        out_specs=pl.BlockSpec(memory_space=pltpu.VMEM),
        scratch_shapes=[
            vm((256, 512), BF16), vm((256, 512), BF16),
            vm((512, 1024), BF16), vm((512, 1024), BF16),
            vm((16, 2, 64, 128), F32), vm((16, 2, 64, 128), BF16),
            vm((16, 64, 256), F32), vm((16, 64, 256), BF16),
            vm((3, 4, 2, 64, 128), BF16), vm((3, 4, 64, 256), BF16),
            vm((4, 2, 64, 128), F32), vm((4, 64, 256), F32), vm((4, 64, 256), BF16),
            vm((3, 64, 128), F32), vm((4, 64, 128), F32), vm((3, 64, 256), BF16),
            vm((2, 4, 4, 2, 2, 64, 128), BF16),
            vm((4, 64, 256), BF16),
            vm((4, 4, 64, 256), BF16),
            vm((2, 2, 64, 256), F32),
            pltpu.SemaphoreType.DMA((7,)),
            pltpu.SemaphoreType.DMA((TOTAL,)),
            pltpu.SemaphoreType.DMA((TOTAL,)),
            pltpu.SemaphoreType.REGULAR,
        ],
        compiler_params=pltpu.CompilerParams(
            collective_id=0, has_side_effects=True, vmem_limit_bytes=40 * 1024 * 1024
        ),
    )(
        *[
            pltpu.with_memory_space_constraint(v, pltpu.HBM)
            for v in (
                activations.reshape(256, 512), gradients.reshape(256, 512), basis_in, basis_out
            )
        ],
        pltpu.with_memory_space_constraint(lengths, pltpu.HBM),
    )


def solution(mesh):
    return jax.shard_map(
        local,
        mesh=mesh,
        in_specs=(
            P(None, "row", "seq"),
            P(None, "col", "seq"),
            P("seq", "col"),
            P("seq", "row"),
            P(),
        ),
        out_specs=P(("row", "seq"), "col"),
        check_vma=False,
    )
```

```python
import jax
import jax.numpy as jnp
from jax import lax
from jax.experimental import pallas as pl
from jax.experimental.pallas import tpu as pltpu
from jax.sharding import PartitionSpec as P

MESH = pl.DeviceIdType.MESH
F32 = jnp.float32
BF16 = jnp.bfloat16

PHASES = dict(
    rs1_in=3, rs1_out=3, rs2_in=7, rs2_out=3, ag1=7, ag2=24, z=3, fw=13
)
FIRST = {}
TOTAL = 0
for _name, _count in PHASES.items():
    FIRST[_name] = TOTAL
    TOTAL += _count


def kernel(
    act_hbm, grad_hbm, bin_hbm, bout_hbm, len_ref, out_ref,
    act, grad, bin_, bout,
    p32_in, p16_in, p32_out, p16_out,
    got_in, got_out,
    q_in, q_out, q16_out, same, cross, got2_out,
    gbuf, obuf, lhs, acc,
    load_sem, send_sem, recv_sem, ready,
):
    s = lax.axis_index("seq")
    r = lax.axis_index("row")
    c = lax.axis_index("col")
    y, x = lax.div(s, 4), lax.rem(s, 4)
    zl, k = lax.div(r, 2), lax.rem(r, 2)
    a = x + k * (y - x)
    b = y + k * (x - y)
    step_a, step_b = 1 + 3 * k, 4 - 3 * k

    def turn(v):
        return lax.rem(v + 4, 4)

    def at(a_, b_):
        return a_ * step_a + b_ * step_b

    started = []

    def send(name, i, src, dst, device):
        n = FIRST[name] + i
        copy = pltpu.make_async_remote_copy(
            src_ref=src, dst_ref=dst, send_sem=send_sem.at[n], recv_sem=recv_sem.at[n],
            device_id=device, device_id_type=MESH,
        )
        copy.start()
        started.append(copy)
        return copy

    def load(i, src, dst):
        copy = pltpu.make_async_copy(src, dst, load_sem.at[i])
        copy.start()
        return copy

    load_act = load(0, act_hbm, act)
    load_bin = [
        load(1 + j, bin_hbm.at[:, pl.ds(256 * j, 256)], bin_.at[:, pl.ds(256 * j, 256)])
        for j in range(4)
    ]
    load_out = [load(5, grad_hbm, grad), load(6, bout_hbm, bout)]

    ap, am, a2 = turn(a + 1), turn(a - 1), turn(a + 2)
    bp, bm, b2 = turn(b + 1), turn(b - 1), turn(b + 2)
    other = 2 * zl + 1 - k
    partner = (s, other, c)
    right, left = (at(ap, b), r, c), (at(am, b), r, c)
    over = 2 * (1 - zl) + k
    far = (at(a2, b), r, c)

    barrier = pltpu.get_barrier_semaphore()

    def greet(s_, row_, c_):
        pl.semaphore_signal(barrier, inc=1, device_id=(s_, row_, c_), device_id_type=MESH)

    for d in (1, 2, 3):
        for s_ in (at(turn(a + d), b), at(a, turn(b + d))):
            greet(s_, 2 * zl, c)
            greet(s_, 2 * (1 - zl) + 1, c)
        greet(s, 2 * zl + 1, turn(c + d))
    greet(s, 2 * (1 - zl) + 1, c)

    @pl.when(k == 1)
    def _():
        greet(s, 2 * zl, c)

    load_act.wait()
    for j in range(4):
        load_bin[j].wait()
        m = jnp.dot(act[...], bin_[:, 256 * j : 256 * (j + 1)], preferred_element_type=F32)
        for h in range(2):
            sc = h + k - 2 * h * k
            for i in range(4):
                blk = m[64 * i : 64 * (i + 1), 128 * h : 128 * (h + 1)]
                at_blk = 4 * j + i + 3 * (i - j) * sc
                p32_in[at_blk, sc] = blk
                p16_in[at_blk, sc] = blk.astype(BF16)

    @pl.when(k == 0)
    def _():
        pl.semaphore_wait(barrier, 13)
        pl.semaphore_signal(ready, inc=1, device_id=partner, device_id_type=MESH)

    @pl.when(k == 1)
    def _():
        pl.semaphore_wait(ready, 1)

    def ring1_start(name, p16, got):
        return [
            send(name, d - 1, p16.at[pl.ds(turn(a + d) * 4, 4)], got.at[d - 1], to)
            for d, to in ((2, far), (1, right), (3, left))
        ]

    def ring1_end(copies, p32, got, q):
        for copy in copies:
            copy.wait_recv()
        q[...] = (
            p32[pl.ds(a * 4, 4)]
            + got[0].astype(F32) + got[1].astype(F32) + got[2].astype(F32)
        )

    rs1_in = ring1_start("rs1_in", p16_in, got_in)

    load_out[0].wait()
    load_out[1].wait()
    for j in range(4):
        m = jnp.dot(grad[...], bout[:, 256 * j : 256 * (j + 1)], preferred_element_type=F32)
        m = m.T
        for i in range(4):
            blk = m[64 * i : 64 * (i + 1)]
            at_blk = 4 * i + j + 3 * (j - i) * k
            p32_out[at_blk] = blk
            p16_out[at_blk] = blk.astype(BF16)
    rs1_out = ring1_start("rs1_out", p16_out, got_out)

    ring1_end(rs1_in, p32_in, got_in, q_in)
    rs2_same, rs2_cross = [], []
    for d in (2, 1, 3):
        to = turn(b + d)
        rs2_same.append(
            send("rs2_in", d - 1, q_in.at[to, 0], same.at[d - 1], (at(a, to), r, c))
        )
        rs2_cross.append(
            send("rs2_in", 3 + d, q_in.at[to, 1], cross.at[d], (at(a, to), other, c))
        )
    rs2_cross.append(send("rs2_in", 3, q_in.at[b, 1], cross.at[0], partner))

    ring1_end(rs1_out, p32_out, got_out, q_out)
    q16_out[...] = q_out[...].astype(BF16)
    rs2_out = [
        send("rs2_out", d - 1, q16_out.at[turn(b + d)], got2_out.at[d - 1], (at(a, turn(b + d)), r, c))
        for d in (2, 1, 3)
    ]

    for copy in rs2_same + rs2_cross:
        copy.wait_recv()
    gbuf[k, a, b, zl, k] = (q_in[b, 0] + same[0] + same[1] + same[2]).astype(BF16)
    gbuf[k, a, b, zl, 1 - k] = (cross[0] + cross[1] + cross[2] + cross[3]).astype(BF16)

    def unit(a_, b_, w):
        return gbuf.at[k, a_, b_, w]

    def own_to(n, b_, row):
        return send("ag1", n, unit(a, b, w0), unit(a, b, w0), (at(a, b_), row, c))

    def along_a(bi, wi):
        b_, w = turn(b + bi), (w0, w1)[wi]
        for d, to in ((2, far), (1, right), (3, left)):
            n = 3 * (4 * wi + bi) + d - 1
            ring_a[bi, wi, d] = send("ag2", n, unit(a, b_, w), unit(a, b_, w), to)

    @pl.when(k == 1)
    def _():
        pl.semaphore_wait(barrier, 20)
        pl.semaphore_signal(ready, inc=1, device_id=partner, device_id_type=MESH)

    @pl.when(k == 0)
    def _():
        pl.semaphore_wait(ready, 1)

    w0, w1 = zl, 1 - zl
    ring_a = {}
    along_a(0, 0)
    near, away = {}, {}
    near[2] = own_to(1, b2, r)
    away[0] = own_to(3, b, over)
    away[2] = own_to(5, b2, over)
    near[1] = own_to(0, bp, r)
    near[3] = own_to(2, bm, r)
    away[1] = own_to(4, bp, over)
    away[3] = own_to(6, bm, over)

    for copy in rs2_out:
        copy.wait_recv()
    obuf[c] = (
        q_out[b] + got2_out[0].astype(F32) + got2_out[1].astype(F32) + got2_out[2].astype(F32)
    ).astype(BF16)

    z = [
        send("z", d - 1, obuf.at[c], obuf.at[c], (s, r, turn(c + d)))
        for d in (2, 1, 3)
    ]

    away[0].wait_recv()
    along_a(0, 1)
    for d in (1, 3):
        near[d].wait_recv()
        along_a(4 - d, 0)
    for d in (1, 3):
        away[d].wait_recv()
        along_a(4 - d, 1)
    near[2].wait_recv()
    along_a(2, 0)
    away[2].wait_recv()
    along_a(2, 1)

    order = (0, 3, 1, 2)
    fw = {0: send("fw", 0, gbuf.at[k, a], gbuf.at[k, a], partner)}

    def forward(bi):
        b_ = turn(b + bi)
        for i, (d, a_) in enumerate(((1, am), (3, ap), (2, a2))):
            for wi in range(2):
                ring_a[bi, wi, d].wait_recv()
            n = 1 + 3 * bi + i
            fw[n] = send("fw", n, gbuf.at[k, a_, b_], gbuf.at[k, a_, b_], partner)

    for bi in order[:3]:
        forward(bi)
    for copy in z:
        copy.wait_recv()

    lane = lax.broadcasted_iota(jnp.int32, (64, 256), 1)
    seq4 = lax.rem(lax.div(lane, 16), 4)
    slot = lax.div(lane, 64) * 16 + lax.rem(lane, 16)
    outs = [obuf[zz].astype(F32) for zz in range(4)]
    for g in range(4):
        whole = jnp.concatenate([v[:, 64 * g : 64 * (g + 1)] for v in outs], axis=1)
        for i in range(4):
            keep = jnp.logical_and(seq4 == i, slot < len_ref[4 * g + i])
            lhs[g, i] = jnp.where(keep, whole, 0.0).astype(BF16)
    forward(order[3])

    acc[...] = jnp.zeros_like(acc)

    def use(part, half, g):
        left_side = lhs[g].reshape(256, 256)
        for pair in range(2):
            right_side = jnp.concatenate(
                [gbuf[half, 2 * pair + i, g].reshape(256, 128) for i in range(2)], axis=1
            )
            prod = jnp.dot(left_side, right_side, preferred_element_type=F32)
            prod = prod * prod
            acc[part, pair] += (prod[:64] + prod[64:128]) + (prod[128:192] + prod[192:])

    fw[0].wait_recv()
    for bi in order:
        use(0, k, turn(b + bi))
        for i in range(3):
            fw[1 + 3 * bi + i].wait_recv()
        use(1, 1 - k, turn(a + bi))

    for part, half in ((0, k), (1, 1 - k)):
        for g in range(4):
            at_col = pl.multiple_of(g * 256 + half * 128, 128)
            out_ref[:, pl.ds(at_col, 128)] = acc[
                part, g // 2, :, 128 * (g % 2) : 128 * (g % 2 + 1)
            ] * (1.0 / 1024.0)

    for copy in started:
        copy.wait_send()


def local(activations, gradients, basis_in, basis_out, lengths):
    hbm = pl.BlockSpec(memory_space=pltpu.HBM)
    vm = pltpu.VMEM
    return pl.pallas_call(
        kernel,
        out_shape=jax.ShapeDtypeStruct((64, 1024), F32),
        in_specs=[hbm] * 4 + [pl.BlockSpec(memory_space=pltpu.SMEM)],
        out_specs=pl.BlockSpec(memory_space=pltpu.VMEM),
        scratch_shapes=[
            vm((256, 512), BF16), vm((256, 512), BF16),
            vm((512, 1024), BF16), vm((512, 1024), BF16),
            vm((16, 2, 64, 128), F32), vm((16, 2, 64, 128), BF16),
            vm((16, 64, 256), F32), vm((16, 64, 256), BF16),
            vm((3, 4, 2, 64, 128), BF16), vm((3, 4, 64, 256), BF16),
            vm((4, 2, 64, 128), F32), vm((4, 64, 256), F32), vm((4, 64, 256), BF16),
            vm((3, 64, 128), F32), vm((4, 64, 128), F32), vm((3, 64, 256), BF16),
            vm((2, 4, 4, 2, 2, 64, 128), BF16),
            vm((4, 64, 256), BF16),
            vm((4, 4, 64, 256), BF16),
            vm((2, 2, 64, 256), F32),
            pltpu.SemaphoreType.DMA((7,)),
            pltpu.SemaphoreType.DMA((TOTAL,)),
            pltpu.SemaphoreType.DMA((TOTAL,)),
            pltpu.SemaphoreType.REGULAR,
        ],
        compiler_params=pltpu.CompilerParams(
            collective_id=0, has_side_effects=True, vmem_limit_bytes=40 * 1024 * 1024
        ),
    )(
        *[
            pltpu.with_memory_space_constraint(v, pltpu.HBM)
            for v in (
                activations.reshape(256, 512), gradients.reshape(256, 512), basis_in, basis_out
            )
        ],
        pltpu.with_memory_space_constraint(lengths, pltpu.HBM),
    )


def solution(mesh):
    return jax.shard_map(
        local,
        mesh=mesh,
        in_specs=(
            P(None, "row", "seq"),
            P(None, "col", "seq"),
            P("seq", "col"),
            P("seq", "row"),
            P(),
        ),
        out_specs=P(("row", "seq"), "col"),
        check_vma=False,
    )
```
